8 devices in a mesh: rep: 1 (over z), tp: 2 (over y), ep: 4 (over x, core).
Axes of the slice: x: 2, y: 2, z: 1, core: 2. Of those that a mesh axis runs over, the one named last changes fastest.
Arguments:
- x_in: bfloat16 [8192, 2048], P(('rep', 'ep'))
- route_ids: int32 [2, 8192, 2], P(None, ('rep', 'ep'))
- gate_vals: float32 [2, 8192, 2], P(None, ('rep', 'ep'))
- w_gate: bfloat16 [2, 4, 2048, 5504], P(None, ('rep', 'ep'), None, 'tp')
- w_up: bfloat16 [2, 4, 2048, 5504], P(None, ('rep', 'ep'), None, 'tp')
- w_down: bfloat16 [2, 4, 5504, 2048], P(None, ('rep', 'ep'), 'tp')
- old_map: int32 [2, 4], replicated
- move_src: int32 [2, 2], replicated
- move_dst: int32 [2, 2], replicated
Outputs:
- output 1: bfloat16 [8192, 2048], P(('rep', 'ep'))
- output 2: bfloat16 [2, 4, 2048, 5504], P(None, ('rep', 'ep'), None, 'tp')
- output 3: bfloat16 [2, 4, 2048, 5504], P(None, ('rep', 'ep'), None, 'tp')
- output 4: bfloat16 [2, 4, 5504, 2048], P(None, ('rep', 'ep'), 'tp')
All inputs are finite; a program needn't handle non-finite values.
Results may differ from the reference program's by a relative error of at most 0.00772671.
Values are sent between devices in bfloat16 or wider.
A program may use at most 1 GiB of HBM per device.

```python
import jax
import jax.numpy as jnp
from jax import lax

MODEL_DIM = 2048
FFN_DIM = 5504
EXPERTS = 4
TOP_K = 2
LOCAL_SLOTS = 1
TOKENS_DEV = 2048
NUM_MOVES = 2
GROUP_SIZE = 4
NUM_LAYERS = 2

NUM_SLOTS = GROUP_SIZE * LOCAL_SLOTS
GROUP_TOKENS = GROUP_SIZE * TOKENS_DEV
CAPACITY = 2 * TOKENS_DEV * TOP_K // NUM_SLOTS
EXPERT_ROWS = GROUP_SIZE * CAPACITY


def device_routes(rng_key):
    hot_count = EXPERTS // 4
    rest_total = TOKENS_DEV * TOP_K - hot_count * CAPACITY
    rest_base = rest_total // (EXPERTS - hot_count)
    rest_extra = rest_total % (EXPERTS - hot_count)
    rank_ids = jnp.arange(EXPERTS, dtype=jnp.int32)
    counts = jnp.where(rank_ids < hot_count, CAPACITY, rest_base + (rank_ids - hot_count < rest_extra).astype(jnp.int32))
    key_label, key_token = jax.random.split(rng_key)
    labels = jax.random.permutation(key_label, EXPERTS).astype(jnp.int32)
    run_ends = jnp.cumsum(counts)
    entries = jnp.arange(TOKENS_DEV * TOP_K, dtype=jnp.int32)
    rank_of = jnp.searchsorted(run_ends, entries, side='right')
    expert_of = labels[rank_of].reshape(TOP_K, TOKENS_DEV).T
    token_order = jax.random.permutation(key_token, TOKENS_DEV)
    return expert_of[token_order]


def layer_maps(rng_key):
    key_extra, key_slot, key_move = jax.random.split(rng_key, 3)
    extra_ids = jax.random.randint(key_extra, (NUM_SLOTS - EXPERTS,), 0, EXPERTS, dtype=jnp.int32)
    slot_expert = jnp.concatenate([jnp.arange(EXPERTS, dtype=jnp.int32), extra_ids])
    slot_perm = jax.random.permutation(key_slot, NUM_SLOTS).astype(jnp.int32)
    old_map = jnp.zeros((NUM_SLOTS,), jnp.int32).at[slot_perm].set(slot_expert)
    chosen = jax.random.permutation(key_move, EXPERTS)[:NUM_MOVES].astype(jnp.int32)
    move_dst = slot_perm[chosen]
    move_src = slot_perm[jnp.roll(chosen, -1)]
    return old_map, move_src, move_dst


def setup_inputs(seed: int = 0, part: int = 0) -> dict:
    root_key = jax.random.key(seed)
    key_shared, key_group = jax.random.split(root_key)
    key_part = jax.random.fold_in(key_group, part)
    old_map, move_src, move_dst = jax.vmap(layer_maps)(jax.random.split(key_shared, NUM_LAYERS))
    key_x, key_route, key_gate, key_wg, key_wu, key_wd = jax.random.split(key_part, 6)
    x_in = jax.random.normal(key_x, (GROUP_TOKENS, MODEL_DIM), jnp.float32).astype(jnp.bfloat16)
    route_ids = jax.vmap(device_routes)(jax.random.split(key_route, NUM_LAYERS * GROUP_SIZE)).reshape(NUM_LAYERS, GROUP_TOKENS, TOP_K)
    gate_vals = jax.random.uniform(key_gate, (NUM_LAYERS, GROUP_TOKENS, TOP_K), jnp.float32, 0.5, 1.5) * TOP_K ** -0.5
    table_gate = (jax.random.normal(key_wg, (NUM_LAYERS, EXPERTS, MODEL_DIM, FFN_DIM), jnp.float32) * MODEL_DIM ** -0.5).astype(jnp.bfloat16)
    table_up = (jax.random.normal(key_wu, (NUM_LAYERS, EXPERTS, MODEL_DIM, FFN_DIM), jnp.float32) * MODEL_DIM ** -0.5).astype(jnp.bfloat16)
    table_down = (jax.random.normal(key_wd, (NUM_LAYERS, EXPERTS, FFN_DIM, MODEL_DIM), jnp.float32) * FFN_DIM ** -0.5).astype(jnp.bfloat16)
    place_slots = jax.vmap(lambda expert_table, slot_map: expert_table[slot_map])
    return {'x_in': x_in, 'route_ids': route_ids, 'gate_vals': gate_vals, 'w_gate': place_slots(table_gate, old_map), 'w_up': place_slots(table_up, old_map), 'w_down': place_slots(table_down, old_map), 'old_map': old_map, 'move_src': move_src, 'move_dst': move_dst}


def moe_layer(hidden, layer_ids, layer_gates, w_gate, w_up, w_down, slot_map):
    first_slot = jax.ops.segment_min(jnp.arange(NUM_SLOTS, dtype=jnp.int32), slot_map, num_segments=EXPERTS)
    flat_ids = layer_ids.reshape(-1)
    sort_order = jnp.argsort(flat_ids, stable=True)
    sorted_tok = (sort_order // TOP_K).astype(jnp.int32)
    sorted_gate = layer_gates.reshape(-1)[sort_order]
    counts = jnp.zeros((EXPERTS,), jnp.int32).at[flat_ids].add(1)
    starts = jnp.cumsum(counts) - counts
    pad_tok = jnp.concatenate([sorted_tok, jnp.zeros((EXPERT_ROWS,), jnp.int32)])
    pad_gate = jnp.concatenate([sorted_gate, jnp.zeros((EXPERT_ROWS,), jnp.float32)])
    row_ids = jnp.arange(EXPERT_ROWS)

    def expert_step(token_acc, expert):
        row_start = starts[expert]
        tok_rows = lax.dynamic_slice(pad_tok, (row_start,), (EXPERT_ROWS,))
        row_gate = jnp.where(row_ids < counts[expert], lax.dynamic_slice(pad_gate, (row_start,), (EXPERT_ROWS,)), 0.0)
        slot_idx = first_slot[expert]
        tok_in = hidden[tok_rows]
        gate_acc = jnp.dot(tok_in, w_gate[slot_idx], preferred_element_type=jnp.float32)
        up_acc = jnp.dot(tok_in, w_up[slot_idx], preferred_element_type=jnp.float32)
        hidden_act = (jax.nn.silu(gate_acc) * up_acc).astype(jnp.bfloat16)
        expert_out = jnp.dot(hidden_act, w_down[slot_idx], preferred_element_type=jnp.float32).astype(jnp.bfloat16)
        token_acc = token_acc.at[tok_rows].add(row_gate[:, None] * expert_out.astype(jnp.float32))
        return token_acc, expert

    token_acc = lax.scan(expert_step, jnp.zeros((GROUP_TOKENS, MODEL_DIM), jnp.float32), jnp.arange(EXPERTS))[0]
    return (hidden.astype(jnp.float32) + token_acc).astype(jnp.bfloat16)


def relocate(weights, move_src, move_dst):
    return jax.vmap(lambda layer_w, src_slot, dst_slot: layer_w.at[dst_slot].set(layer_w[src_slot]))(weights, move_src, move_dst)


def reference(x_in, route_ids, gate_vals, w_gate, w_up, w_down, old_map, move_src, move_dst):
    hidden = x_in
    for layer_idx in range(NUM_LAYERS):
        hidden = moe_layer(hidden, route_ids[layer_idx], gate_vals[layer_idx], w_gate[layer_idx], w_up[layer_idx], w_down[layer_idx], old_map[layer_idx])
    return (hidden, relocate(w_gate, move_src, move_dst), relocate(w_up, move_src, move_dst), relocate(w_down, move_src, move_dst))
```

```python
import jax
import jax.numpy as jnp
from jax import lax
from jax.experimental import pallas as pl
from jax.experimental.pallas import tpu as pltpu
from jax.sharding import PartitionSpec as P


HALF_CHUNK = 256
WEIGHT_CHUNKS = 8
FFN_TILES = 4
INSTALL_TILES = 4


def running_count(mask):
    length = mask.shape[-1]
    blocks = mask.reshape(mask.shape[:-1] + (length // 128, 128)).astype(jnp.bfloat16)
    upper = (jnp.arange(128)[:, None] <= jnp.arange(128)[None, :]).astype(jnp.bfloat16)
    inner = jnp.einsum('...bk,kn->...bn', blocks, upper, preferred_element_type=jnp.float32)
    strict = (jnp.arange(length // 128)[:, None] < jnp.arange(length // 128)[None, :]).astype(jnp.bfloat16)
    before = jnp.einsum('...b,bn->...n', inner[..., -1].astype(jnp.bfloat16), strict, preferred_element_type=jnp.float32)
    return (inner + before[..., None]).reshape(mask.shape).astype(jnp.int32)


def mlp_kernel(rows_ref, gate_ref, up_ref, down_ref, part_ref):
    tile = pl.program_id(0)
    rows = rows_ref[...]
    across = (((1,), (1,)), ((), ()))
    gate_acc = lax.dot_general(rows, gate_ref[0, 0], across, preferred_element_type=jnp.float32)
    up_acc = lax.dot_general(rows, up_ref[0, 0], across, preferred_element_type=jnp.float32)
    act = (jax.nn.silu(gate_acc) * up_acc).astype(jnp.bfloat16)
    part = jnp.dot(act, down_ref[0, 0], preferred_element_type=jnp.float32)

    @pl.when(tile == 0)
    def _():
        part_ref[...] = part

    @pl.when(tile != 0)
    def _():
        part_ref[...] += part


def expert_mlp(rows, gate_t, up_t, down, layer):
    count, width = rows.shape
    columns = down.shape[2]
    tile = columns // FFN_TILES
    weight_spec = pl.BlockSpec((1, 1, tile, width), lambda f: (layer, 0, f, 0))
    row_block = pl.BlockSpec((count, width), lambda f: (0, 0))
    return pl.pallas_call(
        mlp_kernel,
        grid=(FFN_TILES,),
        in_specs=[row_block, weight_spec, weight_spec, weight_spec],
        out_specs=row_block,
        out_shape=jax.ShapeDtypeStruct((count, width), jnp.float32),
        cost_estimate=pl.CostEstimate(flops=6 * count * width * columns, bytes_accessed=6 * width * columns + 8 * count * width, transcendentals=count * columns),
    )(rows, gate_t, up_t, down)


def install_kernel(flags_ref, own_ref, first_ref, back_ref, *refs):
    out_ref = refs[-1]
    tile = pl.program_id(0)
    moved = flags_ref[0] == 1
    from_first = (tile // INSTALL_TILES) == flags_ref[1]

    @pl.when(jnp.logical_not(moved))
    def _():
        out_ref[0, 0] = own_ref[0, 0]

    @pl.when(jnp.logical_and(moved, from_first))
    def _():
        out_ref[0, 0] = first_ref[...]

    @pl.when(jnp.logical_and(moved, jnp.logical_not(from_first)))
    def _():
        out_ref[0, 0] = back_ref[...]


def install(flags, own, first, back, layer, earlier):
    _, _, rows, width = own.shape
    tile = rows // 2 // INSTALL_TILES
    block = (1, 1, tile, width)

    def own_map(t, flags_ref):
        return (layer, 0, jnp.where(flags_ref[0] == 1, 0, t), 0)

    def first_map(t, flags_ref):
        used = jnp.logical_and(flags_ref[0] == 1, (t // INSTALL_TILES) == flags_ref[1])
        return (jnp.where(used, t % INSTALL_TILES, 0), 0)

    def back_map(t, flags_ref):
        used = jnp.logical_and(flags_ref[0] == 1, (t // INSTALL_TILES) != flags_ref[1])
        return (jnp.where(used, t % INSTALL_TILES, 0), 0)

    in_specs = [pl.BlockSpec(block, own_map), pl.BlockSpec((tile, width), first_map), pl.BlockSpec((tile, width), back_map)]
    operands = [flags, own, first, back]
    aliases = {}
    if earlier is not None:
        in_specs.append(pl.BlockSpec(memory_space=pl.ANY))
        operands.append(earlier)
        aliases = {4: 0}
    return pl.pallas_call(
        install_kernel,
        grid_spec=pltpu.PrefetchScalarGridSpec(
            num_scalar_prefetch=1, grid=(2 * INSTALL_TILES,), in_specs=in_specs,
            out_specs=pl.BlockSpec(block, lambda t, flags_ref: (layer, 0, t, 0))),
        out_shape=jax.ShapeDtypeStruct(own.shape, own.dtype),
        input_output_aliases=aliases,
        cost_estimate=pl.CostEstimate(flops=200 * rows * width, bytes_accessed=4 * rows * width, transcendentals=0),
    )(*operands)


def solution(mesh):
    group_size = mesh.shape['ep']
    row_spec = P(('rep', 'ep'), None)
    layer_spec = P(None, ('rep', 'ep'), None)
    col_spec = P(None, ('rep', 'ep'), None, 'tp')
    down_spec = P(None, ('rep', 'ep'), 'tp', None)
    map_spec = P(None, None)

    def over_tp(arr):
        return lax.ppermute(arr, 'tp', [(0, 1), (1, 0)])

    def over_x(arr):
        return lax.ppermute(arr, 'ep', [(i, i ^ 2) for i in range(group_size)])

    def over_core(arr):
        return lax.ppermute(arr, 'ep', [(i, i ^ 1) for i in range(group_size)])

    def device_step(x_in, route_ids, gate_vals, w_gate, w_up, w_down, old_map, move_src, move_dst):
        tokens, width = x_in.shape
        layers = route_ids.shape[0]
        half = tokens // 2
        list_len = group_size * half
        max_chunks = list_len // HALF_CHUNK
        me = lax.axis_index('ep')
        tp = lax.axis_index('tp')
        core = me % 2
        gate_t, up_t = w_gate.swapaxes(2, 3), w_up.swapaxes(2, 3)
        experts = jnp.arange(group_size, dtype=jnp.int32)

        all_ids = lax.all_gather(route_ids, 'ep', axis=1, tiled=True)
        x_in, all_ids = lax.optimization_barrier((x_in, all_ids))
        ids6 = all_ids.reshape(layers, group_size, 2, half, 2)
        chosen = jnp.any(ids6[None] == experts[:, None, None, None, None, None], axis=-1)
        mask = chosen.transpose(1, 3, 0, 2, 4).reshape(layers, 2, group_size, list_len)
        counts = running_count(mask)
        rank = counts - 1
        trips = (jnp.max(counts[..., -1], axis=(1, 2)) + HALF_CHUNK - 1) // HALF_CHUNK

        def expert_lists(layer, my_expert):
            mine = lax.dynamic_index_in_dim(counts[layer], my_expert, axis=1, keepdims=False)
            slots = jnp.arange(list_len, dtype=jnp.int32)
            found = jnp.sum((mine[:, None, :] <= slots[None, :, None]).astype(jnp.int32), axis=-1)
            found = jnp.where(slots[None, :] < mine[:, -1:], found, slots[None, :])
            keep = lax.dynamic_index_in_dim(found, tp, 0, keepdims=False)
            send = lax.dynamic_index_in_dim(found, 1 - tp, 0, keepdims=False)
            return keep, send

        def layer_fn(layer, rows_all, index_of, hidden_half, buffer):
            slot_of = jnp.sum(jnp.where(old_map[layer][None, :] == experts[:, None], experts[None, :], 0), axis=1)
            my_expert = old_map[layer, me]
            keep_list, send_list = expert_lists(layer, my_expert)
            keep_list = index_of(keep_list, tp)
            send_list = index_of(send_list, 1 - tp)
            order = jnp.concatenate([keep_list.reshape(max_chunks, HALF_CHUNK), send_list.reshape(max_chunks, HALF_CHUNK)], axis=1)
            wg, wu, wd = w_gate[layer, 0].T, w_up[layer, 0].T, w_down[layer, 0]

            peer = move_dst[layer, 0] ^ move_dst[layer, 1]
            moved = jnp.any(move_dst[layer] == me)
            in_chip = peer == 1
            halves = [w.reshape(2, w.shape[0] // 2, w.shape[1]) for w in (wg, wu, wd)]
            own_part = [lax.dynamic_index_in_dim(w, core, 0, keepdims=False) for w in halves]
            other_part = [lax.dynamic_index_in_dim(w, 1 - core, 0, keepdims=False) for w in halves]
            from_core = [over_core(w) for w in other_part]
            outgoing = [jnp.where(moved, o, f).reshape(-1, 8, width) for o, f in zip(own_part, from_core)]
            steps = [-(-w.shape[0] // WEIGHT_CHUNKS) for w in outgoing]

            def compute(i):
                idx = lax.dynamic_index_in_dim(order, i, 0, keepdims=False)
                rows = rows_all.at[idx].get(mode='promise_in_bounds')
                part = expert_mlp(rows, gate_t, up_t, w_down, layer)
                return part[:HALF_CHUNK], part[HALF_CHUNK:]

            def put(buffer, i, pair, crossed):
                block = jnp.concatenate([pair, crossed], axis=0)[None]
                return lax.dynamic_update_slice(buffer, block, (jnp.maximum(i, 0), 0, 0, 0))

            def stages(i, carry):
                keep, send, rounded, pair, buffer = carry
                recv = over_tp(send)
                across = over_x(rounded)
                crossed = over_core(pair)
                new_keep, new_send = compute(i)
                buffer = put(buffer, i - 3, pair, crossed)
                return new_keep, new_send, (keep + recv).astype(jnp.bfloat16), jnp.stack([rounded, across]), buffer

            def plain(i, carry):
                return stages(i, carry)

            def with_weights(i, state):
                return with_swap(i, state)

            def with_swap(i, state):
                carry, incoming = state
                landed = []
                for out, inc, step in zip(outgoing, incoming, steps):
                    start = jnp.minimum((i - 1) * step, out.shape[0] - step)
                    piece = over_x(lax.dynamic_slice(out, (start, 0, 0), (step, 8, width)))
                    landed.append(lax.dynamic_update_slice(inc, piece, (start, 0, 0)))
                return stages(i, carry), tuple(landed)

            zero = jnp.zeros((HALF_CHUNK, width), jnp.bfloat16)
            first_keep, first_send = compute(0)
            carry = (first_keep, first_send, zero, jnp.zeros((2, HALF_CHUNK, width), jnp.bfloat16), buffer)
            trip = trips[layer]
            split = jnp.where(in_chip, 1, 1 + WEIGHT_CHUNKS)
            carry, incoming = lax.fori_loop(1, split, with_weights, (carry, tuple(jnp.zeros_like(o) for o in outgoing)))
            carry = lax.fori_loop(split, jnp.maximum(trip, split), plain, carry)
            trip = jnp.maximum(trip, split)
            incoming = [inc.reshape(-1, width) for inc in incoming]
            keep, send, rounded, pair, buffer = carry
            recv = over_tp(send)
            across = over_x(rounded)
            buffer = put(buffer, trip - 3, pair, over_core(pair))
            last = (keep + recv).astype(jnp.bfloat16)
            pair = jnp.stack([rounded, across])
            buffer = put(buffer, trip - 2, pair, over_core(pair))
            pair = jnp.stack([last, over_x(last)])
            buffer = put(buffer, trip - 1, pair, over_core(pair))

            my_ids = lax.dynamic_slice_in_dim(route_ids[layer], tp * half, half, 0)
            my_gates = lax.dynamic_slice_in_dim(gate_vals[layer], tp * half, half, 0)
            my_rank = lax.dynamic_slice(rank[layer], (tp, 0, me * half), (1, group_size, half))[0]
            pos = jnp.sum(jnp.where(my_ids[:, :, None] == experts, my_rank.T[:, None, :], 0), axis=-1)
            relative = slot_of[my_ids] ^ me
            place = (relative % 2) * 2 + relative // 2
            flat = ((pos // HALF_CHUNK) * 4 + place) * HALF_CHUNK + pos % HALF_CHUNK
            table = buffer.reshape(max_chunks * 4 * HALF_CHUNK, width)
            mixture = jnp.zeros((half, width), jnp.float32)
            for j in range(2):
                picked = table.at[flat[:, j]].get(mode='promise_in_bounds')
                mixture = mixture + my_gates[:, j:j + 1] * picked.astype(jnp.float32)
            hidden_next = (hidden_half.astype(jnp.float32) + mixture).astype(jnp.bfloat16)

            back = [over_core(jnp.where(in_chip, o, inc)) for o, inc in zip(own_part, incoming)]
            first = [jnp.where(in_chip, f, inc) for f, inc in zip(from_core, incoming)]
            flags = jnp.stack([moved.astype(jnp.int32), core.astype(jnp.int32)])
            new = (flags, first, back)
            return hidden_next, new, buffer

        relay = 688
        x_half = x_in.reshape(2, half, width)
        my_half = lax.dynamic_index_in_dim(x_half, tp, 0, keepdims=False)
        first = over_x(my_half[:relay])
        rest = over_x(jnp.concatenate([x_half[0, relay:], x_half[1, relay:]], axis=0))
        relayed = over_tp(first)
        sides = jnp.stack([first, relayed])
        low = lax.dynamic_index_in_dim(sides, tp, 0, keepdims=False)
        high = lax.dynamic_index_in_dim(sides, 1 - tp, 0, keepdims=False)
        mid = half - relay
        far = jnp.concatenate([low, rest[:mid], high, rest[mid:]], axis=0)
        near = over_core(x_in)
        far_core = over_core(far)
        rows_all = jnp.concatenate([x_in, near, far, far_core], axis=0)

        def index0(pos, hf):
            home = pos // half
            return (home ^ me) * tokens + hf * half + pos % half

        buffer = jnp.zeros((max_chunks, 4, HALF_CHUNK, width), jnp.bfloat16)
        rows_all, buffer = lax.optimization_barrier((rows_all, buffer))
        h1, (flags, first, back), buffer = layer_fn(0, rows_all, index0, my_half, buffer)
        wholes = (gate_t, up_t, w_down)
        made = [install(flags, w, f, b, 0, None) for w, f, b in zip(wholes, first, back)]

        by_x = over_x(h1)
        by_y = over_tp(h1)
        quarter = half // 2
        xy_low = over_tp(by_x[:quarter])
        xy_high = over_x(by_y[quarter:])
        mine4 = jnp.concatenate([h1, by_x, by_y, xy_low, xy_high], axis=0)
        core4 = over_core(mine4)
        rows_all = jnp.concatenate([mine4, core4], axis=0)

        def index1(pos, hf):
            relative = (pos // half) ^ me
            block = (relative % 2) * 4 + (hf ^ tp) * 2 + relative // 2
            return block * half + pos % half

        h2, (flags, first, back), _ = layer_fn(1, rows_all, index1, h1, buffer)
        h2, made = lax.optimization_barrier((h2, made))
        other = over_tp(h2)
        y_out = jnp.concatenate([jnp.where(tp == 0, h2, other), jnp.where(tp == 0, other, h2)], axis=0)
        new_gate, new_up, new_down = [install(flags, w, f, b, 1, m) for w, f, b, m in zip(wholes, first, back, made)]
        return y_out, new_gate.swapaxes(2, 3), new_up.swapaxes(2, 3), new_down

    return jax.shard_map(device_step, mesh=mesh, in_specs=(row_spec, layer_spec, layer_spec, col_spec, col_spec, down_spec, map_spec, map_spec, map_spec), out_specs=(row_spec, col_spec, col_spec, down_spec), check_vma=False)
```

```python
import jax
import jax.numpy as jnp
from jax import lax
from jax.experimental import pallas as pl
from jax.experimental.pallas import tpu as pltpu
from jax.sharding import PartitionSpec as P


HALF_CHUNK = 256
WEIGHT_CHUNKS = 8
FFN_TILES = 4
INSTALL_TILES = 4
COMBINE_ROWS = 512


def running_count(mask):
    length = mask.shape[-1]
    blocks = mask.reshape(mask.shape[:-1] + (length // 128, 128)).astype(jnp.bfloat16)
    upper = (jnp.arange(128)[:, None] <= jnp.arange(128)[None, :]).astype(jnp.bfloat16)
    inner = jnp.einsum('...bk,kn->...bn', blocks, upper, preferred_element_type=jnp.float32)
    strict = (jnp.arange(length // 128)[:, None] < jnp.arange(length // 128)[None, :]).astype(jnp.bfloat16)
    before = jnp.einsum('...b,bn->...n', inner[..., -1].astype(jnp.bfloat16), strict, preferred_element_type=jnp.float32)
    return (inner + before[..., None]).reshape(mask.shape).astype(jnp.int32)


def mlp_kernel(rows_ref, gate_ref, up_ref, down_ref, part_ref):
    tile = pl.program_id(0)
    rows = rows_ref[...]
    across = (((1,), (1,)), ((), ()))
    gate_acc = lax.dot_general(rows, gate_ref[0, 0], across, preferred_element_type=jnp.float32)
    up_acc = lax.dot_general(rows, up_ref[0, 0], across, preferred_element_type=jnp.float32)
    act = (jax.nn.silu(gate_acc) * up_acc).astype(jnp.bfloat16)
    part = jnp.dot(act, down_ref[0, 0], preferred_element_type=jnp.float32)

    @pl.when(tile == 0)
    def _():
        part_ref[...] = part

    @pl.when(tile != 0)
    def _():
        part_ref[...] += part


def expert_mlp(rows, gate_t, up_t, down, layer):
    count, width = rows.shape
    columns = down.shape[2]
    tile = columns // FFN_TILES
    weight_spec = pl.BlockSpec((1, 1, tile, width), lambda f: (layer, 0, f, 0))
    row_block = pl.BlockSpec((count, width), lambda f: (0, 0))
    return pl.pallas_call(
        mlp_kernel,
        grid=(FFN_TILES,),
        in_specs=[row_block, weight_spec, weight_spec, weight_spec],
        out_specs=row_block,
        out_shape=jax.ShapeDtypeStruct((count, width), jnp.float32),
        cost_estimate=pl.CostEstimate(flops=6 * count * width * columns, bytes_accessed=6 * width * columns + 8 * count * width, transcendentals=count * columns),
    )(rows, gate_t, up_t, down)


def install_kernel(flags_ref, own_ref, first_ref, back_ref, *refs):
    out_ref = refs[-1]
    tile = pl.program_id(0)
    moved = flags_ref[0] == 1
    from_first = (tile // INSTALL_TILES) == flags_ref[1]

    @pl.when(jnp.logical_not(moved))
    def _():
        out_ref[0, 0] = own_ref[0, 0]

    @pl.when(jnp.logical_and(moved, from_first))
    def _():
        out_ref[0, 0] = first_ref[...]

    @pl.when(jnp.logical_and(moved, jnp.logical_not(from_first)))
    def _():
        out_ref[0, 0] = back_ref[...]


def install(flags, own, first, back, layer, earlier):
    _, _, rows, width = own.shape
    tile = rows // 2 // INSTALL_TILES
    block = (1, 1, tile, width)

    def own_map(t, flags_ref):
        return (layer, 0, jnp.where(flags_ref[0] == 1, 0, t), 0)

    def first_map(t, flags_ref):
        used = jnp.logical_and(flags_ref[0] == 1, (t // INSTALL_TILES) == flags_ref[1])
        return (jnp.where(used, t % INSTALL_TILES, 0), 0)

    def back_map(t, flags_ref):
        used = jnp.logical_and(flags_ref[0] == 1, (t // INSTALL_TILES) != flags_ref[1])
        return (jnp.where(used, t % INSTALL_TILES, 0), 0)

    in_specs = [pl.BlockSpec(block, own_map), pl.BlockSpec((tile, width), first_map), pl.BlockSpec((tile, width), back_map)]
    operands = [flags, own, first, back]
    aliases = {}
    if earlier is not None:
        in_specs.append(pl.BlockSpec(memory_space=pl.ANY))
        operands.append(earlier)
        aliases = {4: 0}
    return pl.pallas_call(
        install_kernel,
        grid_spec=pltpu.PrefetchScalarGridSpec(
            num_scalar_prefetch=1, grid=(2 * INSTALL_TILES,), in_specs=in_specs,
            out_specs=pl.BlockSpec(block, lambda t, flags_ref: (layer, 0, t, 0))),
        out_shape=jax.ShapeDtypeStruct(own.shape, own.dtype),
        input_output_aliases=aliases,
        cost_estimate=pl.CostEstimate(flops=200 * rows * width, bytes_accessed=4 * rows * width, transcendentals=0),
    )(*operands)


def solution(mesh):
    group_size = mesh.shape['ep']
    row_spec = P(('rep', 'ep'), None)
    layer_spec = P(None, ('rep', 'ep'), None)
    col_spec = P(None, ('rep', 'ep'), None, 'tp')
    down_spec = P(None, ('rep', 'ep'), 'tp', None)
    map_spec = P(None, None)

    def over_tp(arr):
        return lax.ppermute(arr, 'tp', [(0, 1), (1, 0)])

    def over_x(arr):
        return lax.ppermute(arr, 'ep', [(i, i ^ 2) for i in range(group_size)])

    def over_core(arr):
        return lax.ppermute(arr, 'ep', [(i, i ^ 1) for i in range(group_size)])

    def device_step(x_in, route_ids, gate_vals, w_gate, w_up, w_down, old_map, move_src, move_dst):
        tokens, width = x_in.shape
        layers = route_ids.shape[0]
        half = tokens // 2
        list_len = group_size * half
        max_chunks = list_len // HALF_CHUNK
        me = lax.axis_index('ep')
        tp = lax.axis_index('tp')
        core = me % 2
        gate_t, up_t = w_gate.swapaxes(2, 3), w_up.swapaxes(2, 3)
        experts = jnp.arange(group_size, dtype=jnp.int32)

        all_ids = lax.all_gather(route_ids, 'ep', axis=1, tiled=True)
        x_in, all_ids = lax.optimization_barrier((x_in, all_ids))
        ids6 = all_ids.reshape(layers, group_size, 2, half, 2)
        chosen = jnp.any(ids6[None] == experts[:, None, None, None, None, None], axis=-1)
        mask = chosen.transpose(1, 3, 0, 2, 4).reshape(layers, 2, group_size, list_len)
        counts = running_count(mask)
        rank = counts - 1
        trips = (jnp.max(counts[..., -1], axis=(1, 2)) + HALF_CHUNK - 1) // HALF_CHUNK

        def expert_lists(layer, my_expert):
            mine = lax.dynamic_index_in_dim(counts[layer], my_expert, axis=1, keepdims=False)
            slots = jnp.arange(list_len, dtype=jnp.int32)
            found = jnp.sum((mine[:, None, :] <= slots[None, :, None]).astype(jnp.int32), axis=-1)
            found = jnp.where(slots[None, :] < mine[:, -1:], found, slots[None, :])
            keep = lax.dynamic_index_in_dim(found, tp, 0, keepdims=False)
            send = lax.dynamic_index_in_dim(found, 1 - tp, 0, keepdims=False)
            return keep, send

        def layer_fn(layer, rows_all, index_of, hidden_half, buffer):
            slot_of = jnp.sum(jnp.where(old_map[layer][None, :] == experts[:, None], experts[None, :], 0), axis=1)
            my_expert = old_map[layer, me]
            keep_list, send_list = expert_lists(layer, my_expert)
            keep_list = index_of(keep_list, tp)
            send_list = index_of(send_list, 1 - tp)
            order = jnp.concatenate([keep_list.reshape(max_chunks, HALF_CHUNK), send_list.reshape(max_chunks, HALF_CHUNK)], axis=1)
            wg, wu, wd = w_gate[layer, 0].T, w_up[layer, 0].T, w_down[layer, 0]

            peer = move_dst[layer, 0] ^ move_dst[layer, 1]
            moved = jnp.any(move_dst[layer] == me)
            in_chip = peer == 1
            halves = [w.reshape(2, w.shape[0] // 2, w.shape[1]) for w in (wg, wu, wd)]
            own_part = [lax.dynamic_index_in_dim(w, core, 0, keepdims=False) for w in halves]
            other_part = [lax.dynamic_index_in_dim(w, 1 - core, 0, keepdims=False) for w in halves]
            from_core = [over_core(w) for w in other_part]
            outgoing = [jnp.where(moved, o, f).reshape(-1, 8, width) for o, f in zip(own_part, from_core)]
            steps = [-(-w.shape[0] // WEIGHT_CHUNKS) for w in outgoing]

            def compute(i):
                idx = lax.dynamic_index_in_dim(order, i, 0, keepdims=False)
                rows = rows_all.at[idx].get(mode='promise_in_bounds')
                part = expert_mlp(rows, gate_t, up_t, w_down, layer)
                return part[:HALF_CHUNK], part[HALF_CHUNK:]

            def put(buffer, i, pair, crossed):
                block = jnp.concatenate([pair, crossed], axis=0)[None]
                return lax.dynamic_update_slice(buffer, block, (jnp.maximum(i, 0), 0, 0, 0))

            def stages(i, carry):
                keep, send, rounded, pair, buffer = carry
                recv = over_tp(send)
                across = over_x(rounded)
                crossed = over_core(pair)
                new_keep, new_send = compute(i)
                buffer = put(buffer, i - 3, pair, crossed)
                total = (keep + recv).astype(jnp.bfloat16)
                return new_keep, new_send, total, jnp.stack([rounded, across]), buffer

            def plain(i, carry):
                return stages(i, carry)

            def with_weights(i, state):
                return with_swap(i, state)

            def with_swap(i, state):
                carry, incoming = state
                landed = []
                for out, inc, step in zip(outgoing, incoming, steps):
                    start = jnp.minimum((i - 1) * step, out.shape[0] - step)
                    piece = over_x(lax.dynamic_slice(out, (start, 0, 0), (step, 8, width)))
                    landed.append(lax.dynamic_update_slice(inc, piece, (start, 0, 0)))
                return stages(i, carry), tuple(landed)

            zero = jnp.zeros((HALF_CHUNK, width), jnp.bfloat16)
            first_keep, first_send = compute(0)
            carry = (first_keep, first_send, zero, jnp.zeros((2, HALF_CHUNK, width), jnp.bfloat16), buffer)
            trip = trips[layer]
            split = jnp.where(in_chip, 1, 1 + WEIGHT_CHUNKS)
            carry, incoming = lax.fori_loop(1, split, with_weights, (carry, tuple(jnp.zeros_like(o) for o in outgoing)))
            carry = lax.fori_loop(split, jnp.maximum(trip, split), plain, carry)
            trip = jnp.maximum(trip, split)
            incoming = [inc.reshape(-1, width) for inc in incoming]
            keep, send, rounded, pair, buffer = carry
            recv = over_tp(send)
            across = over_x(rounded)
            buffer = put(buffer, trip - 3, pair, over_core(pair))
            last = (keep + recv).astype(jnp.bfloat16)
            pair = jnp.stack([rounded, across])
            buffer = put(buffer, trip - 2, pair, over_core(pair))
            pair = jnp.stack([last, over_x(last)])
            buffer = put(buffer, trip - 1, pair, over_core(pair))

            my_ids = lax.dynamic_slice_in_dim(route_ids[layer], tp * half, half, 0)
            my_gates = lax.dynamic_slice_in_dim(gate_vals[layer], tp * half, half, 0)
            my_rank = lax.dynamic_slice(rank[layer], (tp, 0, me * half), (1, group_size, half))[0]
            pos = jnp.sum(jnp.where(my_ids[:, :, None] == experts, my_rank.T[:, None, :], 0), axis=-1)
            relative = slot_of[my_ids] ^ me
            place = (relative % 2) * 2 + relative // 2
            flat = ((pos // HALF_CHUNK) * 4 + place) * HALF_CHUNK + pos % HALF_CHUNK
            table = buffer.reshape(max_chunks * 4 * HALF_CHUNK, width)
            blocks = []
            for start in range(0, half, COMBINE_ROWS):
                part = slice(start, start + COMBINE_ROWS)
                first_rows, second_rows = [table.at[flat[part, j]].get(mode='promise_in_bounds').astype(jnp.float32) for j in range(2)]
                mixture = my_gates[part, 0:1] * first_rows + my_gates[part, 1:2] * second_rows
                blocks.append((hidden_half[part].astype(jnp.float32) + mixture).astype(jnp.bfloat16))
            hidden_next = jnp.concatenate(blocks, axis=0)

            back = [over_core(jnp.where(in_chip, o, inc)) for o, inc in zip(own_part, incoming)]
            first = [jnp.where(in_chip, f, inc) for f, inc in zip(from_core, incoming)]
            flags = jnp.stack([moved.astype(jnp.int32), core.astype(jnp.int32)])
            new = (flags, first, back)
            return hidden_next, new, buffer

        relay = 688
        x_half = x_in.reshape(2, half, width)
        my_half = lax.dynamic_index_in_dim(x_half, tp, 0, keepdims=False)
        first = over_x(my_half[:relay])
        rest = over_x(jnp.concatenate([x_half[0, relay:], x_half[1, relay:]], axis=0))
        relayed = over_tp(first)
        sides = jnp.stack([first, relayed])
        low = lax.dynamic_index_in_dim(sides, tp, 0, keepdims=False)
        high = lax.dynamic_index_in_dim(sides, 1 - tp, 0, keepdims=False)
        mid = half - relay
        far = jnp.concatenate([low, rest[:mid], high, rest[mid:]], axis=0)
        near = over_core(x_in)
        far_core = over_core(far)
        rows_all = jnp.concatenate([x_in, near, far, far_core], axis=0)

        def index0(pos, hf):
            home = pos // half
            return (home ^ me) * tokens + hf * half + pos % half

        buffer = jnp.zeros((max_chunks, 4, HALF_CHUNK, width), jnp.bfloat16)
        rows_all, buffer = lax.optimization_barrier((rows_all, buffer))
        h1, (flags, first, back), buffer = layer_fn(0, rows_all, index0, my_half, buffer)
        wholes = (gate_t, up_t, w_down)
        made = [install(flags, w, f, b, 0, None) for w, f, b in zip(wholes, first, back)]

        by_x = over_x(h1)
        by_y = over_tp(h1)
        quarter = half // 2
        xy_low = over_tp(by_x[:quarter])
        xy_high = over_x(by_y[quarter:])
        mine4 = jnp.concatenate([h1, by_x, by_y, xy_low, xy_high], axis=0)
        core4 = over_core(mine4)
        rows_all = jnp.concatenate([mine4, core4], axis=0)

        def index1(pos, hf):
            relative = (pos // half) ^ me
            block = (relative % 2) * 4 + (hf ^ tp) * 2 + relative // 2
            return block * half + pos % half

        h2, (flags, first, back), _ = layer_fn(1, rows_all, index1, h1, buffer)
        h2, made = lax.optimization_barrier((h2, made))
        other = over_tp(h2)
        y_out = jnp.concatenate([jnp.where(tp == 0, h2, other), jnp.where(tp == 0, other, h2)], axis=0)
        new_gate, new_up, new_down = [install(flags, w, f, b, 1, m) for w, f, b, m in zip(wholes, first, back, made)]
        return y_out, new_gate.swapaxes(2, 3), new_up.swapaxes(2, 3), new_down

    return jax.shard_map(device_step, mesh=mesh, in_specs=(row_spec, layer_spec, layer_spec, col_spec, col_spec, down_spec, map_spec, map_spec, map_spec), out_specs=(row_spec, col_spec, col_spec, down_spec), check_vma=False)
```
